32 devices in a mesh: seq: 2 (over core), heads: 4 (over y, x), batch: 4 (over z).
Axes of the slice: x: 2, y: 2, z: 4, core: 2. Of those that a mesh axis runs over, the one named last changes fastest.
Arguments:
- queries: bfloat16 [4, 512, 8192], P('batch', 'seq', 'heads'), may hold values from -160 to 160
- keys: bfloat16 [4, 512, 1024], P('batch', 'seq', 'heads'), may hold values from -7 to 7
- values: bfloat16 [4, 512, 1024], P('batch', 'seq', 'heads'), may hold values from -6 to 6
- doc_lengths: int32 [4, 16], P('batch'), may hold values from 1 to 384, 512 in all within a row
- out_weight: bfloat16 [8192, 8192], P('heads', 'batch'), may hold values from -0.0625 to 0.0625
Outputs:
- projected: bfloat16 [4, 512, 8192], P('heads', 'seq', 'batch')
The draws below stay inside these ranges and needn't reach their ends.
Inputs may be any that keep to these rules, and one draw needn't show every extreme that they name: `doc_lengths`: each row sums to 512; no document is longer than 384 tokens and one is exactly 384.
All inputs are finite; a program needn't handle non-finite values.
Results may differ from the reference program's by a relative error of at most 0.012.
Values may be sent and summed in bfloat16 or wider, within the bound.
No kernel may reach another device: no remote copies, remote signals or barrier semaphores. Data moves between devices by JAX's collectives and lax.ppermute only.
A program may use at most 64 MiB of HBM per device.

```python
import math
import jax
import jax.numpy as jnp
import numpy as np
from jax import lax

QUERY_HEAD_COUNT = 64
VALUE_KEY_HEADS = 8
HEAD_WIDTH = 128
D = 8192
DOCS = 16
QBLOCK = 128
PACKED_BATCH = 4
PACKED_LENGTH = 512
LONGEST = 384


def shared_keys(key):
    sampled_values = jax.random.normal(jax.random.fold_in(key, 11), (PACKED_BATCH, PACKED_LENGTH, VALUE_KEY_HEADS, HEAD_WIDTH), jnp.float32)
    sampled_values = jnp.clip(sampled_values, -6.0, 6.0)
    return sampled_values


def draw_keys(key, part):
    sampled_values = shared_keys(key)
    return sampled_values.reshape(PACKED_BATCH, PACKED_LENGTH, VALUE_KEY_HEADS * HEAD_WIDTH).astype(jnp.bfloat16)


def draw_queries(key, part):
    sampled_values = jax.random.normal(jax.random.fold_in(key, 21), (PACKED_BATCH, PACKED_LENGTH, QUERY_HEAD_COUNT, HEAD_WIDTH), jnp.float32)
    sampled_values = jnp.clip(sampled_values, -6.0, 6.0)
    return sampled_values.reshape(PACKED_BATCH, PACKED_LENGTH, QUERY_HEAD_COUNT * HEAD_WIDTH).astype(jnp.bfloat16)


def level_of(stream_key, dims, shards, low, top_value):
    def one(dim, blocks):
        draws = jax.random.uniform(jax.random.fold_in(jax.random.fold_in(stream_key, 6), dim), (blocks,), jnp.float32, low / len(shards), top_value / len(shards))
        return jnp.repeat(jnp.exp(draws), dims[dim] // blocks).reshape((-1,) + (1,) * (len(dims) - dim - 1))

    loudness = one(*shards[0])
    for cut in shards[1:]:
        loudness = loudness * one(*cut)
    return loudness


def length_profile(count, total, limit, lean):
    portions = [(1 << 20) // math.isqrt(grade ** lean) + 1 for grade in range(2, count + 1)]
    rest, given = total - limit - (count - 1), [1] * (count - 1)
    while rest > 0:
        candidates = [i for i in range(count - 1) if given[i] < limit]
        whole, budget = sum([portions[i] for i in candidates]), rest
        for i in candidates:
            more = min(limit - given[i], max(1, budget * portions[i] // whole), rest)
            given[i] = given[i] + more
            rest = rest - more
    return np.array([limit] + given)


def ragged_sizes(key, count, total, bound, skew):
    if count == 2:
        one = jax.random.randint(key, (), max(1, total - bound), min(bound, total - 1) + 1)
        return jnp.stack([one, total - one])
    tallies = jnp.asarray(length_profile(count, total, bound, skew), jnp.int32)
    twos = (count - 1) // 2
    giver, receiver = tallies[1:1 + 2 * twos:2], tallies[2:2 + 2 * twos:2]
    margin = jnp.minimum(giver - 1, bound - receiver)
    shifted = jax.random.randint(jax.random.fold_in(key, 1), (twos,), 0, 1 << 20) % (margin + 1)
    tallies = tallies.at[1:1 + 2 * twos:2].set(giver - shifted).at[2:2 + 2 * twos:2].set(receiver + shifted)
    return tallies[jax.random.permutation(jax.random.fold_in(key, 2), count)]


def centred(own_key, dims, width, limit, pieces=(), held_as=jnp.bfloat16):
    entries = jax.random.normal(own_key, dims, jnp.float32) * width
    if len(pieces) > 0:
        entries = level_of(own_key, dims, pieces, -0.22, 0.18) * entries
    return jnp.clip(entries, min=-limit, max=limit).astype(held_as)


def setup_inputs(seed: int = 0) -> dict:
    arg_keys = jax.random.split(jax.random.key(seed), 6)
    queries = draw_queries(jax.random.fold_in(arg_keys[5], 71), 0)
    keys = draw_keys(jax.random.fold_in(arg_keys[5], 71), 0)
    values = centred(arg_keys[2], (PACKED_BATCH, PACKED_LENGTH, VALUE_KEY_HEADS * HEAD_WIDTH), 1.0, 6.0, ((0, 4), (1, 2), (2, 4)))
    doc_lengths = jax.vmap(lambda own: ragged_sizes(own, DOCS, PACKED_LENGTH, LONGEST, 2))(jax.random.split(arg_keys[3], PACKED_BATCH)).reshape((PACKED_BATCH, DOCS)).astype(jnp.int32)
    out_weight = centred(arg_keys[4], (QUERY_HEAD_COUNT * HEAD_WIDTH, D), (QUERY_HEAD_COUNT * HEAD_WIDTH) ** -0.5, 0.0625, ((0, 4), (1, 4)))
    return dict(queries=queries, keys=keys, values=values, doc_lengths=doc_lengths, out_weight=out_weight)


def document_of(lengths):
    doc_ends = jnp.cumsum(lengths)
    positions = jnp.arange(PACKED_LENGTH, dtype=jnp.int32)
    return jnp.sum((positions[:, None] >= doc_ends[None, :]).astype(jnp.int32), axis=1)


def attend_sequence(bundle):
    query_sequence, key_sequence, value_sequence, lengths = bundle
    group_width = QUERY_HEAD_COUNT // VALUE_KEY_HEADS
    key_span = min(LONGEST + QBLOCK, PACKED_LENGTH)
    doc_ids = document_of(lengths)
    query_head_rows = query_sequence.reshape(PACKED_LENGTH, VALUE_KEY_HEADS, group_width, HEAD_WIDTH)
    key_head_rows = key_sequence.reshape(PACKED_LENGTH, VALUE_KEY_HEADS, HEAD_WIDTH)
    value_head_rows = value_sequence.reshape(PACKED_LENGTH, VALUE_KEY_HEADS, HEAD_WIDTH)

    def one_block(block_index):
        q_start = (block_index * QBLOCK).astype(jnp.int32)
        k_start = jnp.clip(q_start + QBLOCK - key_span, 0, PACKED_LENGTH - key_span).astype(jnp.int32)
        q_block = lax.dynamic_slice_in_dim(query_head_rows, q_start, QBLOCK, 0).astype(jnp.float32)
        k_block = lax.dynamic_slice_in_dim(key_head_rows, k_start, key_span, 0).astype(jnp.float32)
        v_block = lax.dynamic_slice_in_dim(value_head_rows, k_start, key_span, 0).astype(jnp.float32)
        scores = jnp.einsum("qhgd,khd->hgqk", q_block, k_block, precision=lax.Precision.HIGHEST) * (HEAD_WIDTH ** -0.5)
        q_pos = q_start + jnp.arange(QBLOCK, dtype=jnp.int32)
        k_pos = k_start + jnp.arange(key_span, dtype=jnp.int32)
        q_doc = lax.dynamic_slice_in_dim(doc_ids, q_start, QBLOCK, 0)
        k_doc = lax.dynamic_slice_in_dim(doc_ids, k_start, key_span, 0)
        allowed = (q_doc[:, None] == k_doc[None, :]) & (k_pos[None, :] <= q_pos[:, None])
        scores = jnp.where(allowed, scores, -jnp.inf)
        highest = jnp.max(scores, axis=-1, keepdims=True)
        weights = jnp.exp(scores - highest)
        denominator = jnp.sum(weights, axis=-1)
        rounded = lax.optimization_barrier(weights.astype(jnp.bfloat16)).astype(jnp.float32)
        summed = jnp.einsum("hgqk,khd->qhgd", rounded, v_block, precision=lax.Precision.HIGHEST)
        result = summed / jnp.transpose(denominator, (2, 0, 1))[..., None]
        return result.reshape(QBLOCK, QUERY_HEAD_COUNT * HEAD_WIDTH).astype(jnp.bfloat16)

    outputs = lax.map(one_block, jnp.arange(PACKED_LENGTH // QBLOCK, dtype=jnp.int32))
    return outputs.reshape(PACKED_LENGTH, QUERY_HEAD_COUNT * HEAD_WIDTH)


def reference(queries, keys, values, doc_lengths, out_weight):
    attended = lax.map(attend_sequence, (queries, keys, values, doc_lengths))
    flat_rows = attended.reshape(PACKED_BATCH * PACKED_LENGTH, QUERY_HEAD_COUNT * HEAD_WIDTH).astype(jnp.float32)
    projected = jnp.dot(flat_rows, out_weight.astype(jnp.float32), precision=lax.Precision.HIGHEST)
    return projected.astype(jnp.bfloat16).reshape(PACKED_BATCH, PACKED_LENGTH, D)
```

```python
import functools

import jax
import jax.numpy as jnp
from jax import lax
from jax.experimental import pallas as pl
from jax.experimental.pallas import tpu as pltpu
from jax.sharding import PartitionSpec as P

HEAD_WIDTH = 128
DOCS = 16


def chunk_rows(shard_len):
    quarter = shard_len // 4
    return (quarter, quarter, quarter, shard_len - 3 * quarter)


def attention_kernel(row_starts, row_counts, blocks, shard_len, *refs):
    lengths_ref, q_ref = refs[0], refs[1]
    k_refs = refs[2 : 2 + blocks]
    v_refs = refs[2 + blocks : 2 + 2 * blocks]
    outs = refs[2 + 2 * blocks :]
    kv_heads = k_refs[0].shape[1] // HEAD_WIDTH
    q_groups = q_ref.shape[1] // k_refs[0].shape[1]
    shard_start = lax.axis_index("seq") * shard_len
    factor = HEAD_WIDTH ** (-0.5) * 1.4426950408889634
    for out_ref, row_start, rows in zip(outs, row_starts, row_counts):
        own_count = min(shard_len, -(-(row_start + rows) // 128) * 128)
        counts = [own_count] + [shard_len] * (blocks - 1)
        biases = []
        for distance, count in enumerate(counts):
            t = (
                lax.broadcasted_iota(jnp.int32, (rows, count), 0)
                + (shard_start + row_start)
            )
            u = (
                lax.broadcasted_iota(jnp.int32, (rows, count), 1)
                + (shard_start - distance * shard_len)
            )
            end = jnp.int32(0)
            start = jnp.zeros((rows, count), jnp.int32)
            for d in range(DOCS):
                end = end + lengths_ref[0, d]
                start = jnp.where(t >= end, end, start)
            allowed = (u >= start) & (u <= t)
            biases.append(jnp.where(allowed, 0.0, -jnp.inf).astype(jnp.float32))
        for h in range(kv_heads):
            heads = range(h * q_groups, (h + 1) * q_groups)
            q = jnp.concatenate(
                [
                    q_ref[row_start : row_start + rows, j * HEAD_WIDTH : (j + 1) * HEAD_WIDTH]
                    for j in heads
                ],
                axis=0,
            )
            columns = slice(h * HEAD_WIDTH, (h + 1) * HEAD_WIDTH)
            pieces = []
            for k_ref, count, bias in zip(k_refs, counts, biases):
                s = lax.dot_general(
                    q,
                    k_ref[:count, columns],
                    (((1,), (1,)), ((), ())),
                    preferred_element_type=jnp.float32,
                )
                pieces.append(s.reshape(q_groups, rows, count) + bias[None])
            top = jnp.max(pieces[0], axis=-1, keepdims=True)
            for s in pieces[1:]:
                top = jnp.maximum(top, jnp.max(s, axis=-1, keepdims=True))
            total = None
            summed = None
            for s, v_ref, count in zip(pieces, v_refs, counts):
                w = jnp.exp2((s - top) * factor)
                part = jnp.sum(w, axis=-1, keepdims=True)
                prod = jnp.dot(
                    w.astype(jnp.bfloat16).reshape(q_groups * rows, count),
                    v_ref[:count, columns],
                    preferred_element_type=jnp.float32,
                )
                total = part if total is None else total + part
                summed = prod if summed is None else summed + prod
            result = summed.reshape(q_groups, rows, HEAD_WIDTH) / total
            result = result.astype(jnp.bfloat16)
            for g, j in enumerate(heads):
                out_ref[:, j * HEAD_WIDTH : (j + 1) * HEAD_WIDTH] = result[g]


def attention(lengths, q, ks, vs, row_starts, row_counts):
    shard_len, width = q.shape
    blocks = len(ks)
    vmem = pl.BlockSpec(memory_space=pltpu.VMEM)
    pairs = sum(row_counts) * shard_len * blocks * width
    return pl.pallas_call(
        functools.partial(attention_kernel, row_starts, row_counts, blocks, shard_len),
        out_shape=[jax.ShapeDtypeStruct((r, width), jnp.bfloat16) for r in row_counts],
        in_specs=[pl.BlockSpec(memory_space=pltpu.SMEM), vmem] + [vmem] * (2 * blocks),
        out_specs=[vmem] * len(row_counts),
        cost_estimate=pl.CostEstimate(
            flops=12 * pairs, bytes_accessed=4 * sum(row_counts) * width, transcendentals=0
        ),
        name="attend",
    )(lengths, q, *ks, *vs)


def project_kernel(rows, peers, *refs):
    slots = refs[:peers]
    w_ref = refs[peers]
    outs = refs[peers + 1 : 2 * peers + 1]
    lhs = refs[2 * peers + 1]

    @pl.when(pl.program_id(0) == 0)
    def _():
        mix = lax.axis_index("heads") ^ lax.axis_index("batch")
        for d in range(peers):
            e = mix ^ d
            lhs[pl.ds(pl.multiple_of(e * rows, rows), rows), :] = slots[d][...]

    product = jnp.dot(lhs[...], w_ref[...], preferred_element_type=jnp.float32)
    for e in range(peers):
        outs[e][...] = product[e * rows : (e + 1) * rows].astype(jnp.bfloat16)


def project(slots, weight):
    peers = len(slots)
    rows, depth = slots[0].shape
    width = weight.shape[1]
    tile = min(512, width)
    whole = pl.BlockSpec((rows, depth), lambda n: (0, 0))
    return pl.pallas_call(
        functools.partial(project_kernel, rows, peers),
        grid=(width // tile,),
        out_shape=[jax.ShapeDtypeStruct((rows, width), jnp.bfloat16)] * peers,
        in_specs=[whole] * peers + [pl.BlockSpec((depth, tile), lambda n: (0, n))],
        out_specs=[pl.BlockSpec((rows, tile), lambda n: (0, n))] * peers,
        scratch_shapes=[pltpu.VMEM((peers * rows, depth), jnp.bfloat16)],
        cost_estimate=pl.CostEstimate(
            flops=2 * peers * rows * depth * width,
            bytes_accessed=2 * depth * width,
            transcendentals=0,
        ),
        name="project",
    )(*slots, weight)


def per_device(queries, keys, values, doc_lengths, out_weight):
    shard_len, q_width = queries.shape[1:]
    shards = lax.axis_size("seq")
    z_count = lax.axis_size("batch")
    peers = lax.axis_size("heads")
    longest = shards * shard_len // 2 + shard_len // 2
    reach_back = min((longest + shard_len - 2) // shard_len, shards - 1)
    ks, vs = [keys[0]], [values[0]]
    for distance in range(1, reach_back + 1):
        pairs = [(i, i + distance) for i in range(shards - distance)]
        ks.append(lax.ppermute(keys[0], "seq", pairs))
        vs.append(lax.ppermute(values[0], "seq", pairs))
    counts = chunk_rows(shard_len)
    starts = [sum(counts[:i]) for i in range(len(counts))]
    q = queries[0]
    own = list(attention(doc_lengths, q, ks, vs, starts[:1], counts[:1]))
    own += list(attention(doc_lengths, q, ks, vs, starts[1:], counts[1:]))

    def crossed(x, axis, size, d):
        return lax.ppermute(x, axis, [(i, i ^ d) for i in range(size)])

    z = lax.axis_index("batch")
    output = jnp.zeros((shard_len, out_weight.shape[1]), jnp.bfloat16)
    for block, start, rows in zip(own, starts, counts):
        slots = [block] + [None] * (z_count - 1)
        slots[3] = crossed(block, "batch", z_count, 3)
        slots[1] = crossed(block, "batch", z_count, 1)
        onward = jnp.where((z == 0) | (z == 3), slots[3], block)
        slots[2] = lax.ppermute(onward, "batch", [(0, 1), (3, 2), (1, 3), (2, 0)])
        parts = project(slots, out_weight)
        total = parts[0].astype(jnp.float32)
        for e in range(1, peers):
            total = total + crossed(parts[e], "heads", peers, e).astype(jnp.float32)
        output = lax.dynamic_update_slice(output, total.astype(jnp.bfloat16), (start, 0))
    return output[None]


def solution(mesh):
    return jax.shard_map(
        per_device,
        mesh=mesh,
        in_specs=(
            P("batch", "seq", "heads"),
            P("batch", "seq", "heads"),
            P("batch", "seq", "heads"),
            P("batch", None),
            P("heads", "batch"),
        ),
        out_specs=P("heads", "seq", "batch"),
        check_vma=False,
    )
```

```python
import functools

import jax
import jax.numpy as jnp
from jax import lax
from jax.experimental import pallas as pl
from jax.experimental.pallas import tpu as pltpu
from jax.sharding import PartitionSpec as P


HEAD_WIDTH = 128
DOCS = 16


DIRECT, BOTH = 0, 3
SPLIT = (3, 4, 4, 3, 2)
MODES = (3, 3, 3, 3, 0)


def chunk_rows(shard_len):
    part = shard_len // sum(SPLIT)
    rows = [part * n for n in SPLIT[:-1]]
    return rows + [shard_len - sum(rows)]


def load_kernel(count, *refs):
    sources, targets = refs[:count], refs[count : 2 * count - 1]
    start_ref, lengths_ref, sems = refs[2 * count - 1 :]
    copies = [
        pltpu.make_async_copy(source, target, sems.at[i])
        for i, (source, target) in enumerate(zip(sources, (lengths_ref, *targets)))
    ]
    for copy in copies:
        copy.start()
    copies[0].wait()
    shape = start_ref.shape
    t = lax.broadcasted_iota(jnp.int32, shape, 0) + lax.axis_index("seq") * shape[0]
    end = jnp.int32(0)
    start = jnp.zeros(shape, jnp.int32)
    for d in range(DOCS):
        end = end + lengths_ref[0, d]
        start = jnp.where(t >= end, end, start)
    start_ref[...] = start
    for copy in copies[1:]:
        copy.wait()


def load(lengths, *arrays):
    hbm = pl.BlockSpec(memory_space=pltpu.HBM)
    vmem = pl.BlockSpec(memory_space=pltpu.VMEM)
    sources = [pltpu.with_memory_space_constraint(x, pltpu.HBM) for x in (lengths, *arrays)]
    count = len(sources)
    return pl.pallas_call(
        functools.partial(load_kernel, count),
        out_shape=[pltpu.VMEM(x.shape, x.dtype) for x in arrays]
        + [pltpu.VMEM((arrays[0].shape[0], 128), jnp.int32)],
        in_specs=[hbm] * count,
        out_specs=[vmem] * count,
        scratch_shapes=[
            pltpu.SMEM(lengths.shape, jnp.int32),
            pltpu.SemaphoreType.DMA((count,)),
        ],
        compiler_params=pltpu.CompilerParams(vmem_limit_bytes=8 << 20),
        cost_estimate=pl.CostEstimate(flops=10**6, bytes_accessed=10**6, transcendentals=0),
        name="load",
    )(*sources)


def fetch_kernel(source, target, sem):
    copy = pltpu.make_async_copy(source, target, sem)
    copy.start()
    copy.wait()


def fetch(weight):
    return pl.pallas_call(
        fetch_kernel,
        out_shape=pltpu.VMEM(weight.shape, weight.dtype),
        in_specs=[pl.BlockSpec(memory_space=pltpu.HBM)],
        out_specs=pl.BlockSpec(memory_space=pltpu.VMEM),
        scratch_shapes=[pltpu.SemaphoreType.DMA],
        compiler_params=pltpu.CompilerParams(vmem_limit_bytes=10 << 20),
        cost_estimate=pl.CostEstimate(flops=10**6, bytes_accessed=10**6, transcendentals=0),
        name="fetch",
    )(pltpu.with_memory_space_constraint(weight, pltpu.HBM))


def attention_kernel(row_start, rows, blocks, shard_len, *refs):
    start_ref, q_ref = refs[0], refs[1]
    k_refs = refs[2 : 2 + blocks]
    v_refs = refs[2 + blocks : 2 + 2 * blocks]
    out_ref = refs[2 + 2 * blocks]
    kv_heads = k_refs[0].shape[1] // HEAD_WIDTH
    q_groups = q_ref.shape[1] // k_refs[0].shape[1]
    shard_start = lax.axis_index("seq") * shard_len
    factor = HEAD_WIDTH ** (-0.5) * 1.4426950408889634
    own_count = min(shard_len, -(-(row_start + rows) // 128) * 128)
    counts = [own_count] + [shard_len] * (blocks - 1)
    lo = start_ref[row_start : row_start + rows, :] - shard_start
    t = lax.broadcasted_iota(jnp.int32, (rows, 128), 0) + row_start
    lane = lax.broadcasted_iota(jnp.int32, (rows, 128), 1)
    biases = []
    for distance, count in enumerate(counts):
        parts = []
        for c in range(0, count, 128):
            u = lane + (c - distance * shard_len)
            allowed = (u >= lo) & (u <= t)
            parts.append(jnp.where(allowed, 0.0, -jnp.inf).astype(jnp.float32))
        biases.append(jnp.concatenate(parts, axis=1))
    for h in range(kv_heads):
        heads = range(h * q_groups, (h + 1) * q_groups)
        q = jnp.concatenate(
            [
                q_ref[row_start : row_start + rows, j * HEAD_WIDTH : (j + 1) * HEAD_WIDTH]
                for j in heads
            ],
            axis=0,
        )
        columns = slice(h * HEAD_WIDTH, (h + 1) * HEAD_WIDTH)
        pieces = []
        for k_ref, count, bias in zip(k_refs, counts, biases):
            s = lax.dot_general(
                q,
                k_ref[:count, columns],
                (((1,), (1,)), ((), ())),
                preferred_element_type=jnp.float32,
            )
            pieces.append(s.reshape(q_groups, rows, count) + bias[None])
        top = jnp.max(pieces[0], axis=-1, keepdims=True)
        for s in pieces[1:]:
            top = jnp.maximum(top, jnp.max(s, axis=-1, keepdims=True))
        total = None
        summed = None
        for s, v_ref, count in zip(pieces, v_refs, counts):
            w = jnp.exp2((s - top) * factor)
            part = jnp.sum(w, axis=-1, keepdims=True)
            prod = jnp.dot(
                w.astype(jnp.bfloat16).reshape(q_groups * rows, count),
                v_ref[:count, columns],
                preferred_element_type=jnp.float32,
            )
            total = part if total is None else total + part
            summed = prod if summed is None else summed + prod
        result = summed.reshape(q_groups, rows, HEAD_WIDTH) / total
        result = result.astype(jnp.bfloat16)
        for g, j in enumerate(heads):
            out_ref[:, j * HEAD_WIDTH : (j + 1) * HEAD_WIDTH] = result[g]


def attention(starts, q, ks, vs, row_start, rows):
    shard_len, width = q.shape
    blocks = len(ks)
    vmem = pl.BlockSpec(memory_space=pltpu.VMEM)
    pairs = rows * shard_len * blocks * width
    return pl.pallas_call(
        functools.partial(attention_kernel, row_start, rows, blocks, shard_len),
        out_shape=jax.ShapeDtypeStruct((rows, width), jnp.bfloat16),
        in_specs=[vmem] * (2 + 2 * blocks),
        out_specs=vmem,
        cost_estimate=pl.CostEstimate(
            flops=12 * pairs, bytes_accessed=4 * rows * width, transcendentals=0
        ),
        compiler_params=pltpu.CompilerParams(vmem_limit_bytes=16 << 20),
        name="attend",
    )(starts, q, *ks, *vs)


def project_kernel(peers, mode, *refs):
    slots = refs[:peers]
    w_ref = refs[peers]
    outs = refs[peers + 1 : -1]
    lhs = refs[-1]
    rows = slots[0].shape[0]
    width = w_ref.shape[1]
    owner = lax.axis_index("heads")
    z = lax.axis_index("batch")
    for slot, ahead in zip(slots, (0, peers - 1, 1, 2)):
        e = owner ^ lax.rem(z + ahead, peers)
        lhs[pl.ds(pl.multiple_of(e * rows, rows), rows), :] = slot[...]
    tile = min(512, width // 2)
    for n in range(0, width, tile):
        product = jnp.dot(
            lhs[...], w_ref[:, n : n + tile], preferred_element_type=jnp.float32
        ).astype(jnp.bfloat16)
        for out, offset, kinds in arrangement(mode, outs, width, n):
            for i, e in enumerate(kinds):
                out[i * rows : (i + 1) * rows, offset : offset + tile] = product[
                    e * rows : (e + 1) * rows
                ]


def arrangement(mode, outs, width, n):
    if mode == DIRECT:
        return [(out, n, (e,)) for e, out in enumerate(outs)]
    bit = mode if mode in (1, 2) else (1 if n < width // 2 else 2)
    kept, sent = ((0, 2), (1, 3)) if bit == 1 else ((0, 1), (2, 3))
    if mode in (1, 2):
        return [(outs[0], n, kept), (outs[1], n, sent)]
    at = 0 if bit == 1 else 2
    n -= 0 if bit == 1 else width // 2
    return [(outs[at], n, kept), (outs[at + 1], n, sent)]


def project(slots, weight, mode):
    peers = len(slots)
    rows, depth = slots[0].shape
    width = weight.shape[1]
    if mode == DIRECT:
        shapes = [(rows, width)] * peers
    elif mode == BOTH:
        shapes = [(2 * rows, width // 2)] * 4
    else:
        shapes = [(2 * rows, width)] * 2
    vmem = pl.BlockSpec(memory_space=pltpu.VMEM)
    return pl.pallas_call(
        functools.partial(project_kernel, peers, mode),
        out_shape=[jax.ShapeDtypeStruct(x, jnp.bfloat16) for x in shapes],
        in_specs=[vmem] * (peers + 1),
        out_specs=[vmem] * len(shapes),
        scratch_shapes=[pltpu.VMEM((peers * rows, depth), jnp.bfloat16)],
        cost_estimate=pl.CostEstimate(
            flops=2 * peers * rows * depth * width,
            bytes_accessed=2 * depth * width,
            transcendentals=0,
        ),
        compiler_params=pltpu.CompilerParams(vmem_limit_bytes=20 << 20),
        name="project",
    )(*slots, weight)


def crossed(x, axis, d):
    return lax.ppermute(x, axis, [(i, i ^ d) for i in range(lax.axis_size(axis))])


def gathered(block):
    z = lax.axis_index("batch")
    up = lax.ppermute(block, "batch", [(0, 1), (1, 2), (2, 3), (3, 0)])
    down = lax.ppermute(block, "batch", [(0, 3), (1, 0), (2, 1), (3, 2)])
    onward = jnp.where(z == 0, up, jnp.where(z == 3, down, block))
    across = lax.ppermute(onward, "batch", [(0, 1), (1, 3), (2, 0), (3, 2)])
    return [block, up, down, across]


def added(terms):
    total = terms[0].astype(jnp.float32)
    for term in terms[1:]:
        total = total + term.astype(jnp.float32)
    return total.astype(terms[0].dtype)


def reduced(slots, weight, mode):
    rows = slots[0].shape[0]
    parts = list(project(slots, weight, mode))
    if mode == DIRECT:
        peers = range(1, len(parts))
        terms = parts[:1] + [crossed(parts[e], "heads", e) for e in peers]
        return [added(terms)]
    bits = (1, 2) if mode == BOTH else (mode,)
    came = [crossed(sent, "heads", i) for i, sent in zip(bits, parts[1::2])]
    result = []
    for i, kept, other in zip(bits, parts[::2], came):
        passed = added([kept[rows:], other[rows:]])
        last = crossed(passed, "heads", 3 - i)
        result.append(added([kept[:rows], other[:rows], last]))
    return result


def per_device(queries, keys, values, doc_lengths, out_weight):
    shard_len = queries.shape[1]
    shards = lax.axis_size("seq")
    longest = shards * shard_len // 2 + shard_len // 2
    reach_back = min((longest + shard_len - 2) // shard_len, shards - 1)
    ks, vs = [], []
    for distance in range(1, reach_back + 1):
        pairs = [(i, (i + distance) % shards) for i in range(shards)]
        ks.append(lax.ppermute(keys[0], "seq", pairs))
        vs.append(lax.ppermute(values[0], "seq", pairs))
    q, k0, v0, starts = load(doc_lengths, queries[0], keys[0], values[0])
    weight = fetch(out_weight)
    ks, vs = [k0] + ks, [v0] + vs
    counts = chunk_rows(shard_len)
    at = [sum(counts[:i]) for i in range(len(counts))]
    output = jnp.zeros((shard_len, out_weight.shape[1]), jnp.bfloat16)
    for k, (row, rows) in enumerate(zip(at, counts)):
        block = attention(starts, q, ks, vs, row, rows)
        column = 0
        for part in reduced(gathered(block), weight, MODES[k]):
            output = lax.dynamic_update_slice(output, part, (row, column))
            column += part.shape[1]
    return output[None]


def solution(mesh):
    return jax.shard_map(
        per_device,
        mesh=mesh,
        in_specs=(
            P("batch", "seq", "heads"),
            P("batch", "seq", "heads"),
            P("batch", "seq", "heads"),
            P("batch", None),
            P("heads", "batch"),
        ),
        out_specs=P("heads", "seq", "batch"),
        check_vma=False,
    )
```
